32 devices in a mesh: ctx: 8 (over z, y), tp: 4 (over x, core).
Axes of the slice: x: 2, y: 2, z: 4, core: 2. Of those that a mesh axis runs over, the one named last changes fastest.
Arguments:
- queries: bfloat16 [4096, 4096], P('ctx', 'tp'), may hold values from -22 to 22
- keys: bfloat16 [4096, 512], P('ctx', 'tp'), may hold values from -22 to 22
- values: bfloat16 [4096, 512], P('ctx', 'tp'), may hold values from -36 to 36
- positions: int32 [3, 4096], P(None, 'ctx'), may hold values from 0 to 4095
- segment_ids: int32 [4096], replicated, may hold values from 0 to 3, never falling along the last dimension, each value on 1 to 2048 neighbouring positions
- out_weight: bfloat16 [4096, 8192], P('tp', 'ctx'), may hold values from -0.09375 to 0.09375
- residual: bfloat16 [4096, 8192], P(('ctx', 'tp')), may hold values from -3 to 3
Outputs:
- layer_out: bfloat16 [4096, 8192], P(('ctx', 'tp'))
The draws below stay inside these ranges and needn't reach their ends.
Inputs may be any that keep to these rules, and one draw needn't show every extreme that they name: `segment_ids`: ids never fall along the sequence; each document has 1 to 2048 tokens, and one has exactly 2048.
All inputs are finite; a program needn't handle non-finite values.
Results may differ from the reference program's by a relative error of at most 0.013.
Values may be sent and summed in bfloat16 or wider, within the bound.
A program may use at most 128 MiB of HBM per device.

```python
import math
import jax
import jax.numpy as jnp
import numpy as np
from jax import lax

D = 8192
HD = 128
HQ = 32
HK = 4
DOC = 2048
SEQ = 4096
DOCS = 4
N_TP = 4


def drawn_rows(key, row_count, col_count):
    base_key = jax.random.fold_in(key, 0)
    return jnp.clip(jax.random.normal(base_key, (row_count, col_count), jnp.float32), -6.0, 6.0)


def draw_queries(key, part):
    return drawn_rows(jax.random.fold_in(key, 11), SEQ, HQ * HD).astype(jnp.bfloat16)


def draw_keys(key, part):
    return drawn_rows(jax.random.fold_in(key, 23), SEQ, HK * HD).astype(jnp.bfloat16)


def plant(drawn, stream_key, least, largest):
    index_at = [jax.random.randint(jax.random.fold_in(stream_key, axis), (), 0, length) for axis, length in enumerate(drawn.shape)]
    main_axis = drawn.shape.index(max(drawn.shape))
    beside = index_at[:main_axis] + [(index_at[main_axis] + 1) % drawn.shape[main_axis]] + index_at[main_axis + 1:]
    return drawn.at[tuple(index_at)].set(least).at[tuple(beside)].set(largest)


def levels(key, extent, cuts, least, largest):
    gain = 1.0
    for dim, parts in cuts:
        steps = jax.random.uniform(jax.random.fold_in(jax.random.fold_in(key, 6), dim), (parts,), jnp.float32, least / len(cuts), largest / len(cuts))
        gain = gain * jnp.repeat(jnp.exp(steps), extent[dim] // parts).reshape((-1,) + (1,) * (len(extent) - 1 - dim))
    return gain


def length_profile(count, total, reach, lean):
    portions = [(1 << 20) // math.isqrt(grade ** lean) + 1 for grade in range(2, count + 1)]
    surplus, counts = total - reach - (count - 1), [1] * (count - 1)
    while surplus > 0:
        movable = [i for i in range(count - 1) if counts[i] < reach]
        mass, remaining = sum([portions[i] for i in movable]), surplus
        for i in movable:
            extra = min(reach - counts[i], max(1, remaining * portions[i] // mass), surplus)
            counts[i] = counts[i] + extra
            surplus = surplus - extra
    return np.array([reach] + counts)


def uneven(stream_key, number_of, total, bound, skew):
    if number_of == 2:
        one = jax.random.randint(stream_key, (), max(1, total - bound), min(bound, total - 1) + 1)
        return jnp.stack([one, total - one])
    sizes = jnp.asarray(length_profile(number_of, total, bound, skew), jnp.int32)
    couples = (number_of - 1) // 2
    source_of, receiver = sizes[1:1 + 2 * couples:2], sizes[2:2 + 2 * couples:2]
    margin = jnp.minimum(source_of - 1, bound - receiver)
    moved = jax.random.randint(jax.random.fold_in(stream_key, 1), (couples,), 0, 1 << 20) % (margin + 1)
    sizes = sizes.at[1:1 + 2 * couples:2].set(source_of - moved).at[2:2 + 2 * couples:2].set(receiver + moved)
    return sizes[jax.random.permutation(jax.random.fold_in(stream_key, 2), number_of)]


def noise(stream_key, shape, scale, limit, shards=(), kind=jnp.bfloat16):
    array = jax.random.normal(stream_key, shape, jnp.float32) * scale
    if len(shards) > 0:
        array = levels(stream_key, shape, shards, -0.22, 0.18) * array
    return jnp.clip(array, min=-limit, max=limit).astype(kind)


def setup_inputs(seed: int = 0) -> dict:
    seeds = jax.random.split(jax.random.key(seed), 8)
    return {
        "queries": draw_queries(jax.random.fold_in(seeds[7], 71), 0),
        "keys": draw_keys(jax.random.fold_in(seeds[7], 71), 0),
        "values": noise(seeds[2], (SEQ, HK * HD), 6.0, 36.0, ((0, 8), (1, 4))),
        "positions": plant(jax.random.randint(seeds[3], (3, SEQ), 0, SEQ), jax.random.fold_in(seeds[3], 1), 0, SEQ - 1).astype(jnp.int32),
        "segment_ids": jnp.searchsorted(jnp.cumsum(uneven(seeds[4], DOCS, SEQ, DOC, 1)), jnp.arange(SEQ), side="right").astype(jnp.int32),
        "out_weight": noise(seeds[5], (HQ * HD, D), (HQ * HD) ** -0.5, 0.09375, ((0, 4), (1, 8))),
        "residual": noise(seeds[6], (SEQ, D), 0.5, 3.0, ((0, 32),)),
    }


theta_base = 1000000.0

def rotary_tables(positions):
    half_dim = HD // 2
    freq_index = jnp.arange(half_dim)
    inv_freq = theta_base ** (-2.0 * freq_index.astype(jnp.float32) / HD)
    first_end = HD // 8
    second_end = first_end + 3 * HD // 16
    place = positions.astype(jnp.float32)
    chosen = jnp.where(freq_index[None, :] < first_end, place[0][:, None], jnp.where(freq_index[None, :] < second_end, place[1][:, None], place[2][:, None]))
    angle = chosen * inv_freq[None, :]
    return (jnp.cos(angle), jnp.sin(angle))

def rotate(vectors, cosine_table, sine_table):
    half_dim = HD // 2
    lower_half = vectors[..., :half_dim]
    upper_half = vectors[..., half_dim:]
    cos_b = cosine_table[:, None, :]
    sin_b = sine_table[:, None, :]
    return jnp.concatenate([lower_half * cos_b - upper_half * sin_b, upper_half * cos_b + lower_half * sin_b], axis=-1)

def reference(queries, keys, values, positions, segment_ids, out_weight, residual):
    seq_len = queries.shape[0]
    group_size = HQ // HK
    cosine_table, sine_table = rotary_tables(positions)
    rot_q = rotate(queries.reshape(seq_len, HQ, HD).astype(jnp.float32), cosine_table, sine_table).astype(jnp.bfloat16)
    rot_k = rotate(keys.reshape(seq_len, HK, HD).astype(jnp.float32), cosine_table, sine_table).astype(jnp.bfloat16)
    key_heads = rot_k.transpose(1, 0, 2)
    value_heads = values.reshape(seq_len, HK, HD).transpose(1, 0, 2)
    query_rows = math.gcd(seq_len, 512)
    key_span = min(seq_len, DOC + query_rows)
    score_scale = 1.0 / math.sqrt(HD)

    def one_block(block_index):
        begin = (block_index * query_rows).astype(jnp.int32)
        key_start = jnp.clip(begin + query_rows - key_span, 0, seq_len - key_span).astype(jnp.int32)
        query_block = lax.dynamic_slice_in_dim(rot_q, begin, query_rows, 0)
        query_index = begin + jnp.arange(query_rows, dtype=jnp.int32)
        key_index = key_start + jnp.arange(key_span, dtype=jnp.int32)
        query_seg = lax.dynamic_slice_in_dim(segment_ids, begin, query_rows, 0)
        key_seg = lax.dynamic_slice_in_dim(segment_ids, key_start, key_span, 0)
        allowed = (key_index[None, :] <= query_index[:, None]) & (key_seg[None, :] == query_seg[:, None])
        grouped = query_block.reshape(query_rows, HK, group_size, HD).transpose(1, 0, 2, 3)
        key_part = lax.dynamic_slice_in_dim(key_heads, key_start, key_span, 1)
        value_part = lax.dynamic_slice_in_dim(value_heads, key_start, key_span, 1)

        def one_head(operands):
            query_head, key_head, value_head = operands
            score = jnp.einsum('qgd,nd->gqn', query_head.astype(jnp.float32), key_head.astype(jnp.float32)) * score_scale
            score = jnp.where(allowed[None], score, -1e+30)
            row_peak = lax.optimization_barrier(jnp.max(score, axis=-1, keepdims=True))
            prob = jnp.where(allowed[None], jnp.exp(score - row_peak), 0.0)
            row_sum = lax.optimization_barrier(jnp.sum(prob, axis=-1))
            mixed = jnp.einsum('gqn,nd->gqd', prob.astype(jnp.bfloat16).astype(jnp.float32), value_head.astype(jnp.float32))
            return (mixed / row_sum[..., None]).transpose(1, 0, 2)
        heads_out = lax.map(one_head, (grouped, key_part, value_part))
        return heads_out.transpose(1, 0, 2, 3).reshape(query_rows, HQ * HD)
    blocks = lax.map(one_block, jnp.arange(seq_len // query_rows, dtype=jnp.int32))
    attended = blocks.reshape(seq_len, HQ * HD).astype(jnp.bfloat16)
    part_cols = HQ * HD // N_TP
    summed = residual.astype(jnp.float32)
    for part_index in range(N_TP):
        cols = attended[:, part_index * part_cols:(part_index + 1) * part_cols]
        rows_w = out_weight[part_index * part_cols:(part_index + 1) * part_cols]
        partial_sum = jnp.dot(cols, rows_w, preferred_element_type=jnp.float32).astype(jnp.bfloat16)
        summed = summed + partial_sum.astype(jnp.float32)
    return summed.astype(jnp.bfloat16)
```

```python
import functools
import math

import jax
import jax.numpy as jnp
from jax import lax
from jax.experimental import pallas as pl
from jax.experimental.pallas import tpu as pltpu
from jax.sharding import PartitionSpec as P

HD = 128
DOC = 2048

theta_base = 1000000.0
MESH_ID = pl.DeviceIdType.MESH


def rotary_tables(positions):
    half_dim = HD // 2
    freq_index = jnp.arange(half_dim)
    inv_freq = theta_base ** (-2.0 * freq_index.astype(jnp.float32) / HD)
    first_end = HD // 8
    second_end = first_end + 3 * HD // 16
    place = positions.astype(jnp.float32)
    chosen = jnp.where(
        freq_index[None, :] < first_end,
        place[0][:, None],
        jnp.where(freq_index[None, :] < second_end, place[1][:, None], place[2][:, None]),
    )
    angle = chosen * inv_freq[None, :]
    return (jnp.cos(angle), jnp.sin(angle))


def rotate(vectors, cosine_table, sine_table):
    half_dim = HD // 2
    lower_half = vectors[..., :half_dim]
    upper_half = vectors[..., half_dim:]
    cos_b = cosine_table[:, None, :]
    sin_b = sine_table[:, None, :]
    return jnp.concatenate(
        [lower_half * cos_b - upper_half * sin_b, upper_half * cos_b + lower_half * sin_b], axis=-1
    )


def fused(
    n, inner, reach, tile,
    q_ref, kv_ref, start_ref, w_ref, out_ref,
    kvbuf, wbuf, abuf, bbuf, bias, xsend, xrecv, osend,
    kv_s, kv_r, w_s, w_r, a_s, a_r, f_s, b_r, x_s, x_r, o_s, o_r,
):
    outer = n // inner
    half = inner // 2
    tok = q_ref.shape[0]
    pairs = q_ref.shape[1] // (2 * HD)
    tiles = tok // tile
    span = reach * tok + tile
    rows = tok // 2
    quarter = rows // 2
    cols = w_ref.shape[1]
    c = lax.axis_index("ctx")
    t = lax.axis_index("tp")
    co, ci = c // inner, c % inner
    x, h = t // 2, t % 2
    other_x = 1 - x
    mate = {"ctx": c, "tp": 2 * x + 1 - h}
    across = {"ctx": c, "tp": 2 * other_x + h}

    def remote(src, dst, send, recv, device):
        return pltpu.make_async_remote_copy(
            src_ref=src, dst_ref=dst, send_sem=send, recv_sem=recv,
            device_id=device, device_id_type=MESH_ID,
        )

    def landed(dst, sem):
        pltpu.make_async_copy(dst, dst, sem).wait()

    barrier = pltpu.get_barrier_semaphore()

    def greet(device):
        pl.semaphore_signal(barrier, inc=1, device_id=device, device_id_type=MESH_ID)

    for d in range(1, reach + 1):
        @pl.when(c + d < n)
        def _():
            greet({"ctx": c + d, "tp": t})

        @pl.when(c >= d)
        def _():
            greet({"ctx": c - d, "tp": t})
    for d in range(1, inner):
        for g in range(2):
            greet({"ctx": co * inner + (ci + d) % inner, "tp": 2 * x + g})
    for d in range(1, outer):
        for g in range(2):
            greet({"ctx": (co + d) % outer * inner + ci, "tp": 2 * x + g})
    greet(mate)
    greet(across)
    near = jnp.minimum(reach, n - 1 - c) + jnp.minimum(reach, c)
    pl.semaphore_wait(barrier, near + 2 * (inner - 1) + 2 * (outer - 1) + 2)

    def kv_slot(d):
        return kvbuf.at[:, pl.ds((reach - d) * tok, tok), :]

    def kv_copy(d):
        return remote(kv_ref, kv_slot(d), kv_s.at[d - 1], kv_r.at[d - 1], {"ctx": c + d, "tp": t})

    for d in range(1, reach + 1):
        @pl.when(c + d < n)
        def _():
            kv_copy(d).start()

    owner = ci // half
    w_slot = wbuf.at[h, ci % half]
    w_sem = w_r.at[h, ci % half]

    def w_copy(d):
        device = {"ctx": co * inner + (ci + d) % inner, "tp": 2 * x + owner}
        return remote(w_ref, w_slot, w_s.at[d], w_sem, device)

    for d in range(1, inner):
        w_copy(d).start()

    @pl.when(owner != h)
    def _():
        w_copy(0).start()

    @pl.when(owner == h)
    def _():
        pltpu.make_async_copy(w_ref, w_slot, w_sem).start()

    kvbuf[:, reach * tok:, :] = kv_ref[...]
    for d in range(1, reach + 1):
        @pl.when(c < d)
        def _():
            kvbuf[:, (reach - d) * tok:(reach - d + 1) * tok, :] = jnp.zeros(kv_ref.shape, kv_ref.dtype)

    def fill_bias(rt, _):
        first = start_ref[pl.ds(pl.multiple_of(rt * tile, tile), tile), :] - (
            (c - reach) * tok + rt * tile
        )
        key = lax.broadcasted_iota(jnp.int32, (tile, span), 1)
        query = lax.broadcasted_iota(jnp.int32, (tile, span), 0) + reach * tok
        bias[rt] = jnp.where((key <= query) & (key >= first), 0.0, -1e30).astype(jnp.float32)
        return 0

    lax.fori_loop(0, tiles, fill_bias, 0)

    for d in range(1, reach + 1):
        @pl.when(c >= d)
        def _():
            landed(kv_slot(d), kv_r.at[d - 1])

    factor = math.log2(math.e) / math.sqrt(HD)

    def a_copy(d, hp):
        device = {"ctx": (co + d) % outer * inner + ci, "tp": t}
        return remote(abuf.at[co, hp], abuf.at[co, hp], a_s.at[d, hp], a_r.at[co, hp], device)

    def f_copy(slot, hp):
        return remote(abuf.at[slot, hp], bbuf.at[slot, hp], f_s.at[slot, hp], b_r.at[slot, hp], mate)

    def attend(hp, _):
        def one_tile(rt, _):
            at = pl.ds(pl.multiple_of(rt * tile, tile), tile)
            window = pl.ds(pl.multiple_of(rt * tile, tile), span)
            k = kvbuf[0, window, :]
            v = kvbuf[1, window, :]
            q2 = q_ref[at, pl.ds(pl.multiple_of(hp * 2 * HD, 2 * HD), 2 * HD)]
            done = []
            for e in range(2):
                q = q2[:, e * HD:(e + 1) * HD]
                s = lax.dot_general(
                    q, k, (((1,), (1,)), ((), ())), preferred_element_type=jnp.float32
                ) + bias[rt]
                peak = jnp.max(s, axis=-1, keepdims=True)
                p = jnp.exp2((s - peak) * factor)
                total = jnp.sum(p, axis=-1, keepdims=True)
                mixed = jnp.dot(p.astype(jnp.bfloat16), v, preferred_element_type=jnp.float32)
                done.append((mixed / total).astype(jnp.bfloat16))
            abuf[co, hp, at, :] = jnp.concatenate(done, axis=1)
            return 0

        lax.fori_loop(0, tiles, one_tile, 0)
        for d in range(1, outer):
            a_copy(d, hp).start()
        f_copy(co, hp).start()
        return 0

    lax.fori_loop(0, pairs, attend, 0)

    for i in range(half):
        landed(wbuf.at[0, i], w_r.at[0, i])
        landed(wbuf.at[1, i], w_r.at[1, i])

    def x_copy(slot):
        return remote(xsend.at[slot], xrecv.at[slot], x_s.at[slot], x_r.at[slot], across)

    def o_copy(slot, g):
        device = {"ctx": slot * inner + ci, "tp": 2 * x + g}
        return remote(osend.at[slot, g], out_ref.at[co, h], o_s.at[slot, g], o_r.at[co, h], device)

    def product(slot, side, i):
        at = pl.ds(pl.multiple_of(side * rows, rows), rows)
        mine = jnp.concatenate([abuf[slot, p, at, :] for p in range(pairs)], axis=1)
        theirs = jnp.concatenate([bbuf[slot, p, at, :] for p in range(pairs)], axis=1)
        return jnp.dot(mine, wbuf[h, i], preferred_element_type=jnp.float32) + jnp.dot(
            theirs, wbuf[1 - h, i], preferred_element_type=jnp.float32
        )

    def step(k, _):
        @pl.when((k >= 1) & (k < outer))
        def _():
            slot = (co + k) % outer

            def forward(hp, _):
                landed(abuf.at[slot, hp], a_r.at[slot, hp])
                f_copy(slot, hp).start()
                return 0

            lax.fori_loop(0, pairs, forward, 0)

        @pl.when((k >= 1) & (k <= outer))
        def _():
            slot = (co + k + outer - 1) % outer

            def arrive(hp, _):
                landed(bbuf.at[slot, hp], b_r.at[slot, hp])
                return 0

            lax.fori_loop(0, pairs, arrive, 0)
            for i in range(half):
                xsend[slot, :, i * cols:(i + 1) * cols] = product(slot, other_x, i).astype(jnp.bfloat16)
            x_copy(slot).start()

        @pl.when(k >= 2)
        def _():
            slot = (co + k + outer - 2) % outer
            landed(xrecv.at[slot], x_r.at[slot])
            for i in range(half):
                at = slice(i * cols, (i + 1) * cols)
                both = (product(slot, x, i) + xrecv[slot, :, at].astype(jnp.float32)).astype(jnp.bfloat16)
                osend[slot, 0, :, at] = both[:quarter]
                osend[slot, 1, :, at] = both[quarter:]
            for g in range(2):
                @pl.when((slot != co) | (h != g))
                def _():
                    o_copy(slot, g).start()

                @pl.when((slot == co) & (h == g))
                def _():
                    out_ref[co, h] = osend[slot, g]
        return 0

    lax.fori_loop(0, outer + 2, step, 0)

    for d in range(1, reach + 1):
        @pl.when(c + d < n)
        def _():
            kv_copy(d).wait_send()
    for d in range(1, inner):
        w_copy(d).wait_send()

    @pl.when(owner != h)
    def _():
        w_copy(0).wait_send()

    def drain(slot, _):
        def sent(hp, _):
            f_copy(slot, hp).wait_send()

            @pl.when(slot >= 1)
            def _():
                a_copy(slot, hp).wait_send()
            return 0

        lax.fori_loop(0, pairs, sent, 0)
        x_copy(slot).wait_send()
        for g in range(2):
            @pl.when((slot != co) | (h != g))
            def _():
                o_copy(slot, g).wait_send()
                landed(out_ref.at[slot, g], o_r.at[slot, g])
        return 0

    lax.fori_loop(0, outer, drain, 0)


def on_device(queries, keys, values, positions, segment_ids, out_weight, residual):
    tok = queries.shape[0]
    heads = queries.shape[1] // HD
    n = lax.axis_size("ctx")
    inner = 2 ** max(1, int(math.log2(n)) // 2)
    outer = n // inner
    half = inner // 2
    reach = (DOC + tok - 2) // tok
    tile = math.gcd(tok, 256)
    my_start = lax.axis_index("ctx") * tok
    depth, cols = out_weight.shape
    cosine_table, sine_table = rotary_tables(positions)
    rot_q = rotate(
        queries.reshape(tok, heads, HD).astype(jnp.float32), cosine_table, sine_table
    ).astype(jnp.bfloat16).reshape(tok, heads * HD)
    rot_k = rotate(
        keys.reshape(tok, 1, HD).astype(jnp.float32), cosine_table, sine_table
    ).astype(jnp.bfloat16).reshape(tok, HD)
    pair = jnp.stack([rot_k, values], axis=0)
    my_seg = lax.dynamic_slice_in_dim(segment_ids, my_start, tok, 0)
    start = jnp.sum((segment_ids[None, :] < my_seg[:, None]).astype(jnp.int32), axis=1, keepdims=True)
    pairs = heads // 2
    rows = tok // 2
    wide = half * cols
    bf16 = jnp.bfloat16
    dma = pltpu.SemaphoreType.DMA
    vmem = pl.BlockSpec(memory_space=pltpu.VMEM)
    gathered = pl.pallas_call(
        functools.partial(fused, n, inner, reach, tile),
        out_shape=jax.ShapeDtypeStruct((outer, 2, rows // 2, wide), bf16),
        in_specs=[vmem] * 4,
        out_specs=vmem,
        scratch_shapes=[
            pltpu.VMEM((2, (reach + 1) * tok, HD), bf16),
            pltpu.VMEM((2, half, depth, cols), bf16),
            pltpu.VMEM((outer, pairs, tok, 2 * HD), bf16),
            pltpu.VMEM((outer, pairs, tok, 2 * HD), bf16),
            pltpu.VMEM((tok // tile, tile, reach * tok + tile), jnp.float32),
            pltpu.VMEM((outer, rows, wide), bf16),
            pltpu.VMEM((outer, rows, wide), bf16),
            pltpu.VMEM((outer, 2, rows // 2, wide), bf16),
            dma((reach,)), dma((reach,)),
            dma((inner,)), dma((2, half)),
            dma((outer, pairs)), dma((outer, pairs)),
            dma((outer, pairs)), dma((outer, pairs)),
            dma((outer,)), dma((outer,)),
            dma((outer, 2)), dma((outer, 2)),
        ],
        compiler_params=pltpu.CompilerParams(
            collective_id=0, has_side_effects=True, vmem_limit_bytes=60 * 1024 * 1024
        ),
    )(rot_q, pair, start, out_weight)
    shared = gathered.transpose(2, 0, 1, 3).reshape(residual.shape)
    return (shared.astype(jnp.float32) + residual.astype(jnp.float32)).astype(jnp.bfloat16)


def solution(mesh):
    return jax.shard_map(
        on_device,
        mesh=mesh,
        in_specs=(
            P("ctx", "tp"),
            P("ctx", "tp"),
            P("ctx", "tp"),
            P(None, "ctx"),
            P(),
            P("tp", "ctx"),
            P(("ctx", "tp"), None),
        ),
        out_specs=P(("ctx", "tp"), None),
        check_vma=False,
    )
```

```python
import functools
import math

import jax
import jax.numpy as jnp
from jax import lax
from jax.experimental import pallas as pl
from jax.experimental.pallas import tpu as pltpu
from jax.sharding import PartitionSpec as P

HD = 128
DOC = 2048

theta_base = 1000000.0
MESH_ID = pl.DeviceIdType.MESH


def rotary_tables(positions):
    half_dim = HD // 2
    freq_index = jnp.arange(half_dim)
    inv_freq = theta_base ** (-2.0 * freq_index.astype(jnp.float32) / HD)
    first_end = HD // 8
    second_end = first_end + 3 * HD // 16
    place = positions.astype(jnp.float32)
    chosen = jnp.where(
        freq_index[None, :] < first_end,
        place[0][:, None],
        jnp.where(freq_index[None, :] < second_end, place[1][:, None], place[2][:, None]),
    )
    angle = chosen * inv_freq[None, :]
    return (jnp.cos(angle), jnp.sin(angle))


def rotate(vectors, cosine_table, sine_table):
    half_dim = HD // 2
    lower_half = vectors[..., :half_dim]
    upper_half = vectors[..., half_dim:]
    cos_b = cosine_table[:, None, :]
    sin_b = sine_table[:, None, :]
    return jnp.concatenate(
        [lower_half * cos_b - upper_half * sin_b, upper_half * cos_b + lower_half * sin_b], axis=-1
    )


def fused(
    n, inner, reach, tile,
    q_ref, kv_ref, start_ref, w_ref, out_ref,
    kvbuf, wbuf, abuf, bbuf, bias, xsend, xrecv, osend,
    kv_s, kv_r, w_s, w_r, up_s, down_s, a_r, f_s, b_r, x_s, x_r, o_s, o_r,
):
    outer = n // inner
    half = inner // 2
    tok = q_ref.shape[0]
    pairs = q_ref.shape[1] // (2 * HD)
    tiles = tok // tile
    span = reach * tok + tile
    rows = tok // 2
    quarter = rows // 2
    cols = w_ref.shape[1]
    c = lax.axis_index("ctx")
    t = lax.axis_index("tp")
    co, ci = c // inner, c % inner
    x, h = t // 2, t % 2
    other_x = 1 - x
    mate = {"ctx": c, "tp": 2 * x + 1 - h}
    across = {"ctx": c, "tp": 2 * other_x + h}

    def remote(src, dst, send, recv, device):
        return pltpu.make_async_remote_copy(
            src_ref=src, dst_ref=dst, send_sem=send, recv_sem=recv,
            device_id=device, device_id_type=MESH_ID,
        )

    def landed(dst, sem):
        pltpu.make_async_copy(dst, dst, sem).wait()

    barrier = pltpu.get_barrier_semaphore()

    def greet(device):
        pl.semaphore_signal(barrier, inc=1, device_id=device, device_id_type=MESH_ID)

    for d in range(1, reach + 1):
        @pl.when(c + d < n)
        def _():
            greet({"ctx": c + d, "tp": t})

        @pl.when(c >= d)
        def _():
            greet({"ctx": c - d, "tp": t})
    for d in range(1, inner):
        for g in range(2):
            greet({"ctx": co * inner + (ci + d) % inner, "tp": 2 * x + g})
    for d in range(1, outer):
        for g in range(2):
            greet({"ctx": (co + d) % outer * inner + ci, "tp": 2 * x + g})
    greet(mate)
    greet(across)
    near = jnp.minimum(reach, n - 1 - c) + jnp.minimum(reach, c)
    pl.semaphore_wait(barrier, near + 2 * (inner - 1) + 2 * (outer - 1) + 2)

    def kv_slot(d):
        return kvbuf.at[:, pl.ds((reach - d) * tok, tok), :]

    def kv_copy(d):
        return remote(kv_ref, kv_slot(d), kv_s.at[d - 1], kv_r.at[d - 1], {"ctx": c + d, "tp": t})

    for d in range(1, reach + 1):
        @pl.when(c + d < n)
        def _():
            kv_copy(d).start()

    owner = ci // half
    w_slot = wbuf.at[h, ci % half]
    w_sem = w_r.at[h, ci % half]

    def w_copy(d):
        device = {"ctx": co * inner + (ci + d) % inner, "tp": 2 * x + owner}
        return remote(w_ref, w_slot, w_s.at[d], w_sem, device)

    for d in range(1, inner):
        w_copy(d).start()

    @pl.when(owner != h)
    def _():
        w_copy(0).start()

    @pl.when(owner == h)
    def _():
        pltpu.make_async_copy(w_ref, w_slot, w_sem).start()

    kvbuf[:, reach * tok:, :] = kv_ref[...]
    for d in range(1, reach + 1):
        @pl.when(c < d)
        def _():
            kvbuf[:, (reach - d) * tok:(reach - d + 1) * tok, :] = jnp.zeros(kv_ref.shape, kv_ref.dtype)

    def fill_bias(rt, _):
        first = start_ref[pl.ds(pl.multiple_of(rt * tile, tile), tile), :] - (
            (c - reach) * tok + rt * tile
        )
        key = lax.broadcasted_iota(jnp.int32, (tile, span), 1)
        query = lax.broadcasted_iota(jnp.int32, (tile, span), 0) + reach * tok
        bias[rt] = jnp.where((key <= query) & (key >= first), 0.0, -1e30).astype(jnp.float32)
        return 0

    lax.fori_loop(0, tiles, fill_bias, 0)

    for d in range(1, reach + 1):
        @pl.when(c >= d)
        def _():
            landed(kv_slot(d), kv_r.at[d - 1])

    factor = math.log2(math.e) / math.sqrt(HD)

    def up_copy(slot, hp):
        device = {"ctx": c + inner, "tp": t}
        return remote(abuf.at[slot, hp], abuf.at[slot, hp], up_s.at[slot, hp], a_r.at[slot, hp], device)

    def down_copy(slot, hp):
        device = {"ctx": c - inner, "tp": t}
        return remote(abuf.at[slot, hp], abuf.at[slot, hp], down_s.at[slot, hp], a_r.at[slot, hp], device)

    def f_copy(slot, hp):
        return remote(abuf.at[slot, hp], bbuf.at[slot, hp], f_s.at[slot, hp], b_r.at[slot, hp], mate)

    def pass_on(slot, hp):
        @pl.when((slot <= co) & (co + 1 < outer))
        def _():
            up_copy(slot, hp).start()

        @pl.when((slot >= co) & (co >= 1))
        def _():
            down_copy(slot, hp).start()

        f_copy(slot, hp).start()

    def forward(slot, hp):
        landed(abuf.at[slot, hp], a_r.at[slot, hp])
        pass_on(slot, hp)

    def each_side(distance, action):
        def one_side(side, _):
            slot = co + distance * (2 * side - 1)

            @pl.when((slot >= 0) & (slot < outer) & ((distance > 0) | (side == 1)))
            def _():
                action(slot)
            return 0

        lax.fori_loop(0, 2, one_side, 0)

    def attend(hp, _):
        def one_tile(rt, _):
            at = pl.ds(pl.multiple_of(rt * tile, tile), tile)
            window = pl.ds(pl.multiple_of(rt * tile, tile), span)
            k = kvbuf[0, window, :]
            v = kvbuf[1, window, :]
            q2 = q_ref[at, pl.ds(pl.multiple_of(hp * 2 * HD, 2 * HD), 2 * HD)]
            done = []
            for e in range(2):
                q = q2[:, e * HD:(e + 1) * HD]
                s = lax.dot_general(
                    q, k, (((1,), (1,)), ((), ())), preferred_element_type=jnp.float32
                ) + bias[rt]
                peak = jnp.max(s, axis=-1, keepdims=True)
                p = jnp.exp2((s - peak) * factor)
                total = jnp.sum(p, axis=-1, keepdims=True)
                mixed = jnp.dot(p.astype(jnp.bfloat16), v, preferred_element_type=jnp.float32)
                done.append((mixed / total).astype(jnp.bfloat16))
            abuf[co, hp, at, :] = jnp.concatenate(done, axis=1)
            return 0

        lax.fori_loop(0, tiles, one_tile, 0)
        pass_on(co, hp)

        @pl.when(hp >= lag)
        def _():
            each_side(1, lambda slot: forward(slot, hp - lag))
        return 0

    lag = min(2, pairs)
    lax.fori_loop(0, pairs, attend, 0)

    for i in range(half):
        landed(wbuf.at[0, i], w_r.at[0, i])
        landed(wbuf.at[1, i], w_r.at[1, i])

    def x_copy(slot):
        return remote(xsend.at[slot], xrecv.at[slot], x_s.at[slot], x_r.at[slot], across)

    wide = out_ref.shape[1] // (2 * outer)

    def out_slot(slot, g):
        return out_ref.at[:, pl.ds(pl.multiple_of((slot * 2 + g) * wide, 128), wide)]

    def o_copy(slot, g):
        device = {"ctx": slot * inner + ci, "tp": 2 * x + g}
        return remote(osend.at[slot, g], out_slot(co, h), o_s.at[slot, g], o_r.at[co, h], device)

    def product(slot, side, i):
        at = pl.ds(pl.multiple_of(side * rows, rows), rows)
        mine = jnp.concatenate([abuf[slot, p, at, :] for p in range(pairs)], axis=1)
        theirs = jnp.concatenate([bbuf[slot, p, at, :] for p in range(pairs)], axis=1)
        return jnp.dot(mine, wbuf[h, i], preferred_element_type=jnp.float32) + jnp.dot(
            theirs, wbuf[1 - h, i], preferred_element_type=jnp.float32
        )

    def send_product(slot):
        def arrive(hp, _):
            landed(bbuf.at[slot, hp], b_r.at[slot, hp])
            return 0

        lax.fori_loop(0, pairs, arrive, 0)
        for i in range(half):
            xsend[slot, :, i * cols:(i + 1) * cols] = product(slot, other_x, i).astype(jnp.bfloat16)
        x_copy(slot).start()

    def add_product(slot):
        landed(xrecv.at[slot], x_r.at[slot])
        for i in range(half):
            at = slice(i * cols, (i + 1) * cols)
            both = (product(slot, x, i) + xrecv[slot, :, at].astype(jnp.float32)).astype(jnp.bfloat16)
            osend[slot, 0, :, at] = both[:quarter]
            osend[slot, 1, :, at] = both[quarter:]
        for g in range(2):
            @pl.when((slot != co) | (h != g))
            def _():
                o_copy(slot, g).start()

            @pl.when((slot == co) & (h == g))
            def _():
                out_ref[:, pl.ds(pl.multiple_of((co * 2 + h) * wide, 128), wide)] = osend[slot, g]

    def step(d, _):
        each_side(d - 1, send_product)

        def rest(slot):
            first = jnp.where(d == 1, pairs - lag, 0)

            def one(hp, _):
                forward(slot, hp)
                return 0

            lax.fori_loop(first, pairs, one, 0)

        each_side(d, rest)
        each_side(d - 1, add_product)
        return 0

    lax.fori_loop(1, outer + 1, step, 0)

    for d in range(1, reach + 1):
        @pl.when(c + d < n)
        def _():
            kv_copy(d).wait_send()
    for d in range(1, inner):
        w_copy(d).wait_send()

    @pl.when(owner != h)
    def _():
        w_copy(0).wait_send()

    def drain(slot, _):
        def sent(hp, _):
            f_copy(slot, hp).wait_send()

            @pl.when((slot <= co) & (co + 1 < outer))
            def _():
                up_copy(slot, hp).wait_send()

            @pl.when((slot >= co) & (co >= 1))
            def _():
                down_copy(slot, hp).wait_send()
            return 0

        lax.fori_loop(0, pairs, sent, 0)
        x_copy(slot).wait_send()
        for g in range(2):
            @pl.when((slot != co) | (h != g))
            def _():
                o_copy(slot, g).wait_send()
                landed(out_slot(slot, g), o_r.at[slot, g])
        return 0

    lax.fori_loop(0, outer, drain, 0)


def on_device(queries, keys, values, positions, segment_ids, out_weight, residual):
    tok = queries.shape[0]
    heads = queries.shape[1] // HD
    n = lax.axis_size("ctx")
    inner = 2 ** max(1, int(math.log2(n)) // 2)
    outer = n // inner
    half = inner // 2
    reach = (DOC + tok - 2) // tok
    tile = math.gcd(tok, 256)
    my_start = lax.axis_index("ctx") * tok
    depth, cols = out_weight.shape
    cosine_table, sine_table = rotary_tables(positions)
    rot_q = rotate(
        queries.reshape(tok, heads, HD).astype(jnp.float32), cosine_table, sine_table
    ).astype(jnp.bfloat16).reshape(tok, heads * HD)
    rot_k = rotate(
        keys.reshape(tok, 1, HD).astype(jnp.float32), cosine_table, sine_table
    ).astype(jnp.bfloat16).reshape(tok, HD)
    pair = jnp.stack([rot_k, values], axis=0)
    my_seg = lax.dynamic_slice_in_dim(segment_ids, my_start, tok, 0)
    start = jnp.sum((segment_ids[None, :] < my_seg[:, None]).astype(jnp.int32), axis=1, keepdims=True)
    pairs = heads // 2
    rows = tok // 2
    wide = half * cols
    bf16 = jnp.bfloat16
    dma = pltpu.SemaphoreType.DMA
    vmem = pl.BlockSpec(memory_space=pltpu.VMEM)
    gathered = pl.pallas_call(
        functools.partial(fused, n, inner, reach, tile),
        out_shape=jax.ShapeDtypeStruct((rows // 2, outer * 2 * wide), bf16),
        in_specs=[vmem] * 4,
        out_specs=vmem,
        scratch_shapes=[
            pltpu.VMEM((2, (reach + 1) * tok, HD), bf16),
            pltpu.VMEM((2, half, depth, cols), bf16),
            pltpu.VMEM((outer, pairs, tok, 2 * HD), bf16),
            pltpu.VMEM((outer, pairs, tok, 2 * HD), bf16),
            pltpu.VMEM((tok // tile, tile, reach * tok + tile), jnp.float32),
            pltpu.VMEM((outer, rows, wide), bf16),
            pltpu.VMEM((outer, rows, wide), bf16),
            pltpu.VMEM((outer, 2, rows // 2, wide), bf16),
            dma((reach,)), dma((reach,)),
            dma((inner,)), dma((2, half)),
            dma((outer, pairs)),
            dma((outer, pairs)), dma((outer, pairs)),
            dma((outer, pairs)), dma((outer, pairs)),
            dma((outer,)), dma((outer,)),
            dma((outer, 2)), dma((outer, 2)),
        ],
        compiler_params=pltpu.CompilerParams(
            collective_id=0, has_side_effects=True, vmem_limit_bytes=60 * 1024 * 1024
        ),
    )(rot_q, pair, start, out_weight)
    return (gathered.astype(jnp.float32) + residual.astype(jnp.float32)).astype(jnp.bfloat16)


def solution(mesh):
    return jax.shard_map(
        on_device,
        mesh=mesh,
        in_specs=(
            P("ctx", "tp"),
            P("ctx", "tp"),
            P("ctx", "tp"),
            P(None, "ctx"),
            P(),
            P("tp", "ctx"),
            P(("ctx", "tp"), None),
        ),
        out_specs=P(("ctx", "tp"), None),
        check_vma=False,
    )
```

```python
import functools
import math

import jax
import jax.numpy as jnp
from jax import lax
from jax.experimental import pallas as pl
from jax.experimental.pallas import tpu as pltpu
from jax.sharding import PartitionSpec as P

HD = 128
DOC = 2048

theta_base = 1000000.0
MESH_ID = pl.DeviceIdType.MESH


def rotary_tables(positions):
    half_dim = HD // 2
    freq_index = jnp.arange(half_dim)
    inv_freq = theta_base ** (-2.0 * freq_index.astype(jnp.float32) / HD)
    first_end = HD // 8
    second_end = first_end + 3 * HD // 16
    place = positions.astype(jnp.float32)
    chosen = jnp.where(
        freq_index[None, :] < first_end,
        place[0][:, None],
        jnp.where(freq_index[None, :] < second_end, place[1][:, None], place[2][:, None]),
    )
    angle = chosen * inv_freq[None, :]
    return (jnp.cos(angle), jnp.sin(angle))


def rotate(vectors, cosine_table, sine_table):
    half_dim = HD // 2
    lower_half = vectors[..., :half_dim]
    upper_half = vectors[..., half_dim:]
    cos_b = cosine_table[:, None, :]
    sin_b = sine_table[:, None, :]
    return jnp.concatenate(
        [lower_half * cos_b - upper_half * sin_b, upper_half * cos_b + lower_half * sin_b], axis=-1
    )


def fused(
    n, inner, reach, tile,
    q_ref, kv_ref, start_ref, w_ref, out_ref,
    kvbuf, wbuf, abuf, bbuf, bias, xsend, xrecv, osend,
    kv_s, kv_r, w_s, w_r, up_s, down_s, a_r, f_s, b_r, x_s, x_r, o_s, o_r,
):
    outer = n // inner
    half = inner // 2
    tok = q_ref.shape[0]
    pairs = q_ref.shape[1] // (2 * HD)
    tiles = tok // tile
    span = reach * tok + tile
    rows = tok // 2
    quarter = rows // 2
    cols = w_ref.shape[1]
    c = lax.axis_index("ctx")
    t = lax.axis_index("tp")
    co, ci = c // inner, c % inner
    x, h = t // 2, t % 2
    other_x = 1 - x
    mate = {"ctx": c, "tp": 2 * x + 1 - h}
    across = {"ctx": c, "tp": 2 * other_x + h}

    def remote(src, dst, send, recv, device):
        return pltpu.make_async_remote_copy(
            src_ref=src, dst_ref=dst, send_sem=send, recv_sem=recv,
            device_id=device, device_id_type=MESH_ID,
        )

    def landed(dst, sem):
        pltpu.make_async_copy(dst, dst, sem).wait()

    barrier = pltpu.get_barrier_semaphore()

    def greet(device):
        pl.semaphore_signal(barrier, inc=1, device_id=device, device_id_type=MESH_ID)

    for d in range(1, reach + 1):
        @pl.when(c + d < n)
        def _():
            greet({"ctx": c + d, "tp": t})

        @pl.when(c >= d)
        def _():
            greet({"ctx": c - d, "tp": t})
    for d in range(1, inner):
        for g in range(2):
            greet({"ctx": co * inner + (ci + d) % inner, "tp": 2 * x + g})
    for d in range(1, outer):
        for g in range(2):
            greet({"ctx": (co + d) % outer * inner + ci, "tp": 2 * x + g})
    greet(mate)
    greet(across)
    near = jnp.minimum(reach, n - 1 - c) + jnp.minimum(reach, c)
    pl.semaphore_wait(barrier, near + 2 * (inner - 1) + 2 * (outer - 1) + 2)

    def kv_slot(d):
        return kvbuf.at[:, pl.ds((reach - d) * tok, tok), :]

    def kv_copy(d):
        return remote(kv_ref, kv_slot(d), kv_s.at[d - 1], kv_r.at[d - 1], {"ctx": c + d, "tp": t})

    for d in range(1, reach + 1):
        @pl.when(c + d < n)
        def _():
            kv_copy(d).start()

    owner = ci // half
    w_slot = wbuf.at[h, ci % half]
    w_sem = w_r.at[h, ci % half]

    def w_copy(d):
        device = {"ctx": co * inner + (ci + d) % inner, "tp": 2 * x + owner}
        return remote(w_ref, w_slot, w_s.at[d], w_sem, device)

    for d in range(1, inner):
        w_copy(d).start()

    @pl.when(owner != h)
    def _():
        w_copy(0).start()

    @pl.when(owner == h)
    def _():
        pltpu.make_async_copy(w_ref, w_slot, w_sem).start()

    kvbuf[:, reach * tok:, :] = kv_ref[...]
    for d in range(1, reach + 1):
        @pl.when(c < d)
        def _():
            kvbuf[:, (reach - d) * tok:(reach - d + 1) * tok, :] = jnp.zeros(kv_ref.shape, kv_ref.dtype)

    def fill_bias(rt, _):
        first = start_ref[pl.ds(pl.multiple_of(rt * tile, tile), tile), :] - (
            (c - reach) * tok + rt * tile
        )
        key = lax.broadcasted_iota(jnp.int32, (tile, span), 1)
        query = lax.broadcasted_iota(jnp.int32, (tile, span), 0) + reach * tok
        bias[rt] = jnp.where((key <= query) & (key >= first), 0.0, -1e30).astype(jnp.float32)
        return 0

    lax.fori_loop(0, tiles, fill_bias, 0)

    for d in range(1, reach + 1):
        @pl.when(c >= d)
        def _():
            landed(kv_slot(d), kv_r.at[d - 1])

    factor = math.log2(math.e) / math.sqrt(HD)

    def up_copy(slot, hp):
        device = {"ctx": c + inner, "tp": t}
        return remote(abuf.at[slot, hp], abuf.at[slot, hp], up_s.at[slot, hp], a_r.at[slot, hp], device)

    def down_copy(slot, hp):
        device = {"ctx": c - inner, "tp": t}
        return remote(abuf.at[slot, hp], abuf.at[slot, hp], down_s.at[slot, hp], a_r.at[slot, hp], device)

    def f_copy(slot, hp):
        return remote(abuf.at[slot, hp], bbuf.at[slot, hp], f_s.at[slot, hp], b_r.at[slot, hp], mate)

    def pass_on(slot, hp):
        @pl.when((slot <= co) & (co + 1 < outer))
        def _():
            up_copy(slot, hp).start()

        @pl.when((slot >= co) & (co >= 1))
        def _():
            down_copy(slot, hp).start()

        f_copy(slot, hp).start()

    def forward(slot, hp):
        landed(abuf.at[slot, hp], a_r.at[slot, hp])
        pass_on(slot, hp)

    def each_side(distance, action):
        def one_side(side, _):
            slot = co + distance * (2 * side - 1)

            @pl.when((slot >= 0) & (slot < outer) & ((distance > 0) | (side == 1)))
            def _():
                action(slot)
            return 0

        lax.fori_loop(0, 2, one_side, 0)

    def attend(hp, _):
        def one_tile(rt, _):
            at = pl.ds(pl.multiple_of(rt * tile, tile), tile)
            window = pl.ds(pl.multiple_of(rt * tile, tile), span)
            k = kvbuf[0, window, :]
            v = kvbuf[1, window, :]
            q2 = q_ref[at, pl.ds(pl.multiple_of(hp * 2 * HD, 2 * HD), 2 * HD)]
            done = []
            for e in range(2):
                q = q2[:, e * HD:(e + 1) * HD]
                s = lax.dot_general(
                    q, k, (((1,), (1,)), ((), ())), preferred_element_type=jnp.float32
                ) + bias[rt]
                peak = jnp.max(s, axis=-1, keepdims=True)
                p = jnp.exp2((s - peak) * factor)
                total = jnp.sum(p, axis=-1, keepdims=True)
                mixed = jnp.dot(p.astype(jnp.bfloat16), v, preferred_element_type=jnp.float32)
                done.append((mixed / total).astype(jnp.bfloat16))
            abuf[co, hp, at, :] = jnp.concatenate(done, axis=1)
            return 0

        lax.fori_loop(0, tiles, one_tile, 0)
        pass_on(co, hp)

        @pl.when(hp >= lag)
        def _():
            each_side(1, lambda slot: forward(slot, hp - lag))
        return 0

    lag = min(1, pairs)
    lax.fori_loop(0, pairs, attend, 0)

    for i in range(half):
        landed(wbuf.at[0, i], w_r.at[0, i])
        landed(wbuf.at[1, i], w_r.at[1, i])

    def x_copy(slot):
        return remote(xsend.at[slot], xrecv.at[slot], x_s.at[slot], x_r.at[slot], across)

    wide = out_ref.shape[1] // (2 * outer)

    def out_slot(slot, g):
        return out_ref.at[:, pl.ds(pl.multiple_of((slot * 2 + g) * wide, 128), wide)]

    def o_copy(slot, g):
        device = {"ctx": slot * inner + ci, "tp": 2 * x + g}
        return remote(osend.at[slot, g], out_slot(co, h), o_s.at[slot, g], o_r.at[co, h], device)

    def product(slot, side, i):
        at = pl.ds(pl.multiple_of(side * rows, rows), rows)
        mine = jnp.concatenate([abuf[slot, p, at, :] for p in range(pairs)], axis=1)
        theirs = jnp.concatenate([bbuf[slot, p, at, :] for p in range(pairs)], axis=1)
        return jnp.dot(mine, wbuf[h, i], preferred_element_type=jnp.float32) + jnp.dot(
            theirs, wbuf[1 - h, i], preferred_element_type=jnp.float32
        )

    def send_product(slot):
        def arrive(hp, _):
            landed(bbuf.at[slot, hp], b_r.at[slot, hp])
            return 0

        lax.fori_loop(0, pairs, arrive, 0)
        for i in range(half):
            xsend[slot, :, i * cols:(i + 1) * cols] = product(slot, other_x, i).astype(jnp.bfloat16)
        x_copy(slot).start()

    def add_product(slot):
        landed(xrecv.at[slot], x_r.at[slot])
        for i in range(half):
            at = slice(i * cols, (i + 1) * cols)
            both = (product(slot, x, i) + xrecv[slot, :, at].astype(jnp.float32)).astype(jnp.bfloat16)
            osend[slot, 0, :, at] = both[:quarter]
            osend[slot, 1, :, at] = both[quarter:]
        for g in range(2):
            @pl.when((slot != co) | (h != g))
            def _():
                o_copy(slot, g).start()

            @pl.when((slot == co) & (h == g))
            def _():
                out_ref[:, pl.ds(pl.multiple_of((co * 2 + h) * wide, 128), wide)] = osend[slot, g]

    def step(d, _):
        each_side(d - 1, send_product)

        def rest(slot):
            first = jnp.where(d == 1, pairs - lag, 0)

            def one(hp, _):
                forward(slot, hp)
                return 0

            lax.fori_loop(first, pairs, one, 0)

        each_side(d, rest)
        each_side(d - 1, add_product)
        return 0

    lax.fori_loop(1, outer + 1, step, 0)

    for d in range(1, reach + 1):
        @pl.when(c + d < n)
        def _():
            kv_copy(d).wait_send()
    for d in range(1, inner):
        w_copy(d).wait_send()

    @pl.when(owner != h)
    def _():
        w_copy(0).wait_send()

    def drain(slot, _):
        def sent(hp, _):
            f_copy(slot, hp).wait_send()

            @pl.when((slot <= co) & (co + 1 < outer))
            def _():
                up_copy(slot, hp).wait_send()

            @pl.when((slot >= co) & (co >= 1))
            def _():
                down_copy(slot, hp).wait_send()
            return 0

        lax.fori_loop(0, pairs, sent, 0)
        x_copy(slot).wait_send()
        for g in range(2):
            @pl.when((slot != co) | (h != g))
            def _():
                o_copy(slot, g).wait_send()
                landed(out_slot(slot, g), o_r.at[slot, g])
        return 0

    lax.fori_loop(0, outer, drain, 0)


def on_device(queries, keys, values, positions, segment_ids, out_weight, residual):
    tok = queries.shape[0]
    heads = queries.shape[1] // HD
    n = lax.axis_size("ctx")
    inner = 2 ** max(1, int(math.log2(n)) // 2)
    outer = n // inner
    half = inner // 2
    reach = (DOC + tok - 2) // tok
    tile = math.gcd(tok, 256)
    my_start = lax.axis_index("ctx") * tok
    depth, cols = out_weight.shape
    cosine_table, sine_table = rotary_tables(positions)
    rot_q = rotate(
        queries.reshape(tok, heads, HD).astype(jnp.float32), cosine_table, sine_table
    ).astype(jnp.bfloat16).reshape(tok, heads * HD)
    rot_k = rotate(
        keys.reshape(tok, 1, HD).astype(jnp.float32), cosine_table, sine_table
    ).astype(jnp.bfloat16).reshape(tok, HD)
    pair = jnp.stack([rot_k, values], axis=0)
    my_seg = lax.dynamic_slice_in_dim(segment_ids, my_start, tok, 0)
    start = jnp.sum((segment_ids[None, :] < my_seg[:, None]).astype(jnp.int32), axis=1, keepdims=True)
    pairs = heads // 2
    rows = tok // 2
    wide = half * cols
    bf16 = jnp.bfloat16
    dma = pltpu.SemaphoreType.DMA
    vmem = pl.BlockSpec(memory_space=pltpu.VMEM)
    gathered = pl.pallas_call(
        functools.partial(fused, n, inner, reach, tile),
        out_shape=jax.ShapeDtypeStruct((rows // 2, outer * 2 * wide), bf16),
        in_specs=[vmem] * 4,
        out_specs=vmem,
        scratch_shapes=[
            pltpu.VMEM((2, (reach + 1) * tok, HD), bf16),
            pltpu.VMEM((2, half, depth, cols), bf16),
            pltpu.VMEM((outer, pairs, tok, 2 * HD), bf16),
            pltpu.VMEM((outer, pairs, tok, 2 * HD), bf16),
            pltpu.VMEM((tok // tile, tile, reach * tok + tile), jnp.float32),
            pltpu.VMEM((outer, rows, wide), bf16),
            pltpu.VMEM((outer, rows, wide), bf16),
            pltpu.VMEM((outer, 2, rows // 2, wide), bf16),
            dma((reach,)), dma((reach,)),
            dma((inner,)), dma((2, half)),
            dma((outer, pairs)),
            dma((outer, pairs)), dma((outer, pairs)),
            dma((outer, pairs)), dma((outer, pairs)),
            dma((outer,)), dma((outer,)),
            dma((outer, 2)), dma((outer, 2)),
        ],
        compiler_params=pltpu.CompilerParams(
            collective_id=0, has_side_effects=True, vmem_limit_bytes=60 * 1024 * 1024
        ),
    )(rot_q, pair, start, out_weight)
    return (gathered.astype(jnp.float32) + residual.astype(jnp.float32)).astype(jnp.bfloat16)


def solution(mesh):
    return jax.shard_map(
        on_device,
        mesh=mesh,
        in_specs=(
            P("ctx", "tp"),
            P("ctx", "tp"),
            P("ctx", "tp"),
            P(None, "ctx"),
            P(),
            P("tp", "ctx"),
            P(("ctx", "tp"), None),
        ),
        out_specs=P(("ctx", "tp"), None),
        check_vma=False,
    )
```
